32 devices in a mesh: tissue: 2 (over core), row: 4 (over y, x), col: 4 (over z).
Axes of the slice: x: 2, y: 2, z: 4, core: 2. Of those that a mesh axis runs over, the one named last changes fastest.
Arguments:
- expr: float32 [1200, 16384], P(('tissue', 'row'), 'col'), parts along dimension 0, may hold values from -48 to 88
- win_genes: int32 [256], replicated, may hold values from 0 to 16383, as said below
Outputs:
- margin: float32 [512, 16384], P(('tissue', 'row'), 'col'), parts along dimension 0
- degree: float32 [32768], P(('tissue', 'col')), parts along dimension 0
The draws below stay inside these ranges and needn't reach their ends.
There are 2 independent parts, one for each index of `tissue`. The reference program is written for one: setup_inputs(seed, part) draws one part's arguments, and reference() takes and returns one part's arrays. A program takes and returns all parts, laid end to end along the dimension named above; an argument that names none is the same for every part. Nothing has to cross between parts.
Inputs may be any that keep to these rules, and one draw needn't show every extreme that they name: `win_genes`: 256 distinct gene numbers.
All inputs are finite; a program needn't handle non-finite values.
Results may differ from the reference program's by a relative error of at most 0.00077.
Values may be sent and summed in bfloat16 or wider, within the bound.
A program may use at most 128 MiB of HBM per device.

```python
import jax
import jax.numpy as jnp
from jax import lax

G = 16384
S = 600
WIN = 256
N_COL = 4


factor_count = 24


def draw_expr(key, part):
    keys = jax.random.split(jax.random.fold_in(key, 11), 7)
    factors = jax.random.truncated_normal(keys[0], -4.0, 4.0, (S, factor_count), jnp.float32)
    module = jax.random.randint(keys[1], (G,), 0, factor_count)
    sign = jnp.where(jax.random.randint(keys[2], (G,), 0, 2) == 0, -1.0, 1.0)
    load = jax.random.uniform(keys[3], (G,), jnp.float32, 0.4, 1.6) * sign
    loads = jax.random.normal(keys[4], (factor_count, G), jnp.float32) * 0.15
    loads = loads + jax.nn.one_hot(module, factor_count, dtype=jnp.float32).T * load[None, :]
    noise_scale = jax.random.uniform(keys[5], (G,), jnp.float32, 0.3, 1.2)
    noise = jax.random.normal(keys[6], (S, G), jnp.float32)
    signal = jnp.dot(factors, loads, precision=lax.Precision.HIGHEST) + noise * noise_scale[None, :]
    signal = jnp.clip(signal, -12.0, 12.0)
    return signal


def draw_win_genes(key, part):
    order = jax.random.permutation(jax.random.fold_in(key, 23), G)
    return order[:WIN].astype(jnp.int32)


def setup_inputs(seed: int = 0, part: int = 0) -> dict:
    streams_of = jax.random.split(jax.random.key(seed), 3)
    own_keys = jax.random.split(jax.random.fold_in(streams_of[2], part), 3)
    return {
        "expr": draw_expr(jax.random.fold_in(jax.random.fold_in(streams_of[2], part), 71), part),
        "win_genes": draw_win_genes(jax.random.fold_in(streams_of[2], 71), part),
    }


def power_eight(corr):
    half = (1.0 + corr) * 0.5
    half = half * half
    half = half * half
    return half * half

def reference(expr, win_genes):
    mean = lax.optimization_barrier(jnp.sum(expr, axis=0)) / S
    centered = expr - mean
    squares = lax.optimization_barrier(jnp.sum(centered * centered, axis=0))
    z = (centered / jnp.sqrt(squares + 1e-06)).astype(jnp.bfloat16)
    zwin = jnp.take(z, win_genes.astype(jnp.int32), axis=1)
    panel = power_eight(jnp.dot(zwin.T, z, preferred_element_type=jnp.float32)).astype(jnp.bfloat16)
    width = G // N_COL

    def column(start):
        block = lax.dynamic_slice_in_dim(z, start, width, 1)
        adj = power_eight(jnp.dot(z.T, block, preferred_element_type=jnp.float32)).astype(jnp.bfloat16)
        rows_id = jnp.arange(G, dtype=jnp.int32)
        cols_id = start + jnp.arange(width, dtype=jnp.int32)
        keep = rows_id[:, None] != cols_id[None, :]
        degree = lax.optimization_barrier(jnp.sum(jnp.where(keep, adj.astype(jnp.float32), jnp.float32(0.0)), axis=0))
        margin = jnp.dot(panel, adj, preferred_element_type=jnp.float32)
        return (margin, degree)
    starts = jnp.arange(N_COL, dtype=jnp.int32) * width
    blocks, degrees = lax.map(column, starts)
    margin = jnp.transpose(blocks, (1, 0, 2)).reshape(WIN, G)
    return (margin, degrees.reshape(G))
```

```python
import functools

import jax
import jax.numpy as jnp
from jax import lax
from jax.experimental import pallas as pl
from jax.experimental.pallas import tpu as pltpu
from jax.sharding import PartitionSpec as P

MESH = pl.DeviceIdType.MESH
F32 = jnp.float32
BF16 = jnp.bfloat16


def power_eight(corr):
    half = (1.0 + corr) * 0.5
    half = half * half
    half = half * half
    return half * half


def flip(r, d):
    out = r
    for b in range(6):
        bit = 1 << b
        out = out + ((d // bit) % 2) * (1 - 2 * ((r // bit) % 2)) * bit
    return out


def dot(a, b, dims=((1,), (0,))):
    return lax.dot_general(a, b, (dims, ((), ())), preferred_element_type=F32)


def kernel(R, C, eps, expr, win, out, dego,
           stats, zl, zcol, zrt, zw, zwr, zwt, zt, pbuf, macc, rs, degb, degr,
           s_st, r_st, s_aa, r_aa, s_ga, r_ga, s_zc, r_zc, s_zr, r_zr,
           s_up, r_up, s_dn, r_dn, s_rs, r_rs, s_dg, r_dg):
    r = lax.axis_index("row")
    c = lax.axis_index("col")
    S, width = expr.shape
    pad = zl.shape[0]
    slab = width // R
    W = zw.shape[2]
    per = W // R
    NC, chunk = zrt.shape[1], zrt.shape[2]

    barrier = pltpu.get_barrier_semaphore()
    for d in range(1, R):
        pl.semaphore_signal(barrier, inc=1, device_id={"row": flip(r, d)}, device_id_type=MESH)
    for d in range(1, C):
        pl.semaphore_signal(barrier, inc=1, device_id={"col": lax.rem(c + d, C)}, device_id_type=MESH)

    for j in range(R):
        cols = slice(j * slab, (j + 1) * slab)
        x = expr[:, cols]
        total = jnp.sum(x, axis=0, keepdims=True)
        dev = x - total * (1.0 / S)
        stats[0, 0:1, cols] = total
        stats[0, 1:2, cols] = jnp.sum(dev * dev, axis=0, keepdims=True)
    pl.semaphore_wait(barrier, R + C - 2)

    def rowcopy(src, dst, ss, rr, d):
        return pltpu.make_async_remote_copy(
            src_ref=src, dst_ref=dst, send_sem=ss, recv_sem=rr,
            device_id={"row": flip(r, d)}, device_id_type=MESH)

    def colcopy(src, dst, ss, rr, peer):
        return pltpu.make_async_remote_copy(
            src_ref=src, dst_ref=dst, send_sem=ss, recv_sem=rr,
            device_id={"col": peer}, device_id_type=MESH)

    st = [rowcopy(stats.at[0], stats.at[d], s_st.at[d], r_st.at[d], d) for d in range(1, R)]
    for cp in st:
        cp.start()
    macc[...] = jnp.zeros_like(macc)
    zl[pad - 16:pad, :] = jnp.zeros((16, width), BF16)
    pbuf[...] = jnp.ones_like(pbuf)
    for cp in st:
        cp.wait_recv()

    for j in range(R):
        cols = slice(j * slab, (j + 1) * slab)
        total = stats[0, 0:1, cols]
        for d in range(1, R):
            total = total + stats[d, 0:1, cols]
        mean = total / (S * R)
        sq = jnp.zeros_like(mean)
        for d in range(R):
            gap = stats[d, 0:1, cols] * (1.0 / S) - mean
            sq = sq + (stats[d, 1:2, cols] + S * gap * gap)
        inv = 1.0 / jnp.sqrt(sq + eps)
        zl[0:S, cols] = ((expr[:, cols] - mean) * inv).astype(BF16)

    mine = pl.ds(pl.multiple_of(r * pad, 16), pad)
    aa = []
    for d in range(1, R):
        q = flip(r, d)
        aa.append(rowcopy(zl.at[:, pl.ds(pl.multiple_of(q * slab, 128), slab)],
                          zcol.at[q, mine, :], s_aa.at[d], r_aa.at[d], d))
        aa[-1].start()
    zcol[r, mine, :] = zl[:, pl.ds(pl.multiple_of(r * slab, 128), slab)]

    pick = jnp.zeros((pad, W), F32)
    for j in range(R):
        gene = lax.broadcasted_iota(jnp.int32, (slab, W), 0) + (c * width + j * slab)
        onehot = jnp.where(gene == win[...], 1.0, 0.0).astype(BF16)
        pick = pick + dot(zl[:, j * slab:(j + 1) * slab], onehot)
    zw[0] = pick.astype(BF16)
    zc = []
    for d in range(1, C):
        zc.append(colcopy(zw.at[0], zw.at[d], s_zc.at[d], r_zc.at[d], lax.rem(c + d, C)))
        zc[-1].start()

    for cp in aa:
        cp.wait_recv()
    zr_own = zcol.at[r]
    lo, hi = c > 0, c < C - 1

    def up(s, k):
        i = c - s
        return colcopy(zrt.at[i, k], zrt.at[i, k], s_up.at[s, k], r_up.at[s, k], c + 1)

    def up_in(s, k):
        i = c - s
        return colcopy(zrt.at[i, k], zrt.at[i, k], s_up.at[s - 1, k], r_up.at[s - 1, k], c + 1)

    def down(s, k):
        i = c + s
        return colcopy(zrt.at[i, k], zrt.at[i, k], s_dn.at[s, k], r_dn.at[s, k], c - 1)

    def down_in(s, k):
        i = c + s
        return colcopy(zrt.at[i, k], zrt.at[i, k], s_dn.at[s - 1, k], r_dn.at[s - 1, k], c - 1)

    for k in range(NC):
        zrt[c, k] = zr_own[:, k * chunk:(k + 1) * chunk].T

        @pl.when(hi)
        def _():
            up(0, k).start()

        @pl.when(lo)
        def _():
            down(0, k).start()

    ga = []
    for d in range(1, R):
        ga.append(rowcopy(zcol.at[r], zcol.at[r], s_ga.at[d], r_ga.at[d], d))

    tot = zw[0].astype(F32)
    for cp in zc:
        cp.wait_recv()
    for d in range(1, C):
        tot = tot + zw[d].astype(F32)
    zwr[0] = tot.astype(BF16)
    zr = []
    for d in range(1, R):
        zr.append(rowcopy(zwr.at[0], zwr.at[d], s_zr.at[d], r_zr.at[d], d))
        zr[-1].start()
    for cp in ga:
        cp.start()
    for cp in zr:
        cp.wait_recv()
    for d in range(R):
        zwt[pl.ds(pl.multiple_of(flip(r, d) * pad, 16), pad), :] = zwr[d]
    zt[...] = zwt[...].T

    def compute(i, k, d_lo, d_hi):
        pbuf[0:W, :] = power_eight(dot(zt[...], zrt[i, k], ((1,), (1,)))).astype(BF16)

        def one(d, _):
            j = flip(r, d)
            adj = power_eight(dot(zrt[i, k], zcol[j])).astype(BF16)
            macc[j] += dot(pbuf[...], adj)
            return 0
        lax.fori_loop(d_lo, d_hi, one, 0)

    def arrive(s, k):
        @pl.when(c - s >= 0)
        def _():
            up_in(s, k).wait_recv()

            @pl.when(hi)
            def _():
                up(s, k).start()

        @pl.when(c + s < C)
        def _():
            down_in(s, k).wait_recv()

            @pl.when(lo)
            def _():
                down(s, k).start()

    def phase(s, t_lo, t_hi, start, d_hi):
        def step(k, _):
            arrive(s, k)

            def each(t, _):
                i = c + (1 - 2 * (t % 2)) * ((t + 1) // 2)

                @pl.when((i >= 0) & (i < C))
                def _():
                    compute(i, k, start(t), d_hi)
                return 0
            lax.fori_loop(t_lo, t_hi, each, 0)
            return 0
        lax.fori_loop(0, NC, step, 0)

    def own(k, _):
        compute(c, k, 0, 1)
        return 0
    lax.fori_loop(0, NC, own, 0)

    def pass_on(k, _):
        arrive(1, k)
        return 0
    lax.fori_loop(0, NC, pass_on, 0)
    for cp in ga[:-1]:
        cp.wait_recv()
    phase(2, 0, 3, lambda t: jnp.where(t == 0, 1, 0), R - 1)
    ga[-1].wait_recv()
    phase(3, 0, 7, lambda t: jnp.where(t < 3, R - 1, 0), R)
    if C > 4:
        def later(s, _):
            phase(s, 2 * s - 1, 2 * s + 1, lambda t: 0, R)
            return 0
        lax.fori_loop(4, C, later, 0)

    out_cp = []
    for d in range(1, R):
        q = pl.multiple_of(flip(r, d) * per, 8)
        for j in range(R):
            out_cp.append(rowcopy(macc.at[j, pl.ds(q, per), :], rs.at[d, j],
                                  s_rs.at[d, j], r_rs.at[d, j], d))
            out_cp[-1].start()
    for j in range(R):
        degb[j] = macc[j, W:W + 1, :]
    zs = zcol[r].astype(F32)
    self_term = power_eight(jnp.sum(zs * zs, axis=0, keepdims=True))
    degb[r] = degb[r] - self_term.astype(BF16).astype(F32)
    dg = []
    for d in range(1, R):
        dg.append(rowcopy(degb, degr.at[d], s_dg.at[d], r_dg.at[d], d))
        dg[-1].start()
    own_rows = pl.ds(pl.multiple_of(r * per, 8), per)
    for j in range(R):
        total = macc[j, own_rows, :]
        for d in range(1, R):
            out_cp[(d - 1) * R + j].wait_recv()
            total = total + rs[d, j]
        out[:, j * slab:(j + 1) * slab] = total
    for cp in dg:
        cp.wait_recv()
    for j in range(R):
        total = degb[j]
        for d in range(1, R):
            total = total + degr[d, j]
        dego[:, j * slab:(j + 1) * slab] = total

    for cp in st + aa + zc + zr + ga + out_cp + dg:
        cp.wait_send()

    def drain(s, _):
        def each(k, _):
            @pl.when(hi & (c - s >= 0))
            def _():
                up(s, k).wait_send()

            @pl.when(lo & (c + s < C))
            def _():
                down(s, k).wait_send()
            return 0
        lax.fori_loop(0, NC, each, 0)
        return 0
    lax.fori_loop(0, C - 1, drain, 0)


def solution(mesh):
    R, C = mesh.shape["row"], mesh.shape["col"]

    def body(expr, win):
        S, width = expr.shape
        W = win.shape[0]
        pad = (S + 15) // 16 * 16
        slab = width // R
        chunk = min(256, slab)
        NC = slab // chunk
        V = pltpu.VMEM
        dma = pltpu.SemaphoreType.DMA
        vm = pl.BlockSpec(memory_space=pltpu.VMEM)
        margin, degree = pl.pallas_call(
            functools.partial(kernel, R, C, 1e-6),
            out_shape=(jax.ShapeDtypeStruct((W // R, width), F32),
                       jax.ShapeDtypeStruct((1, width), F32)),
            in_specs=[vm, vm],
            out_specs=(vm, vm),
            scratch_shapes=[
                V((R, 2, width), F32),
                V((pad, width), BF16),
                V((R, R * pad, slab), BF16),
                V((C, NC, chunk, R * pad), BF16),
                V((C, pad, W), BF16),
                V((R, pad, W), BF16),
                V((R * pad, W), BF16),
                V((W, R * pad), BF16),
                V((W + 16, chunk), BF16),
                V((R, W + 16, slab), F32),
                V((R, R, W // R, slab), F32),
                V((R, 1, slab), F32),
                V((R, R, 1, slab), F32),
                dma((R,)), dma((R,)), dma((R,)), dma((R,)), dma((R,)), dma((R,)),
                dma((C,)), dma((C,)), dma((R,)), dma((R,)),
                dma((C, NC)), dma((C, NC)), dma((C, NC)), dma((C, NC)),
                dma((R, R)), dma((R, R)), dma((R,)), dma((R,)),
            ],
            compiler_params=pltpu.CompilerParams(
                collective_id=0, has_side_effects=True, vmem_limit_bytes=56 << 20),
        )(expr, win.reshape(1, W))
        return margin, degree.reshape(width)

    in_specs = (P(("tissue", "row"), "col"), P())
    out_specs = (P(("tissue", "row"), "col"), P(("tissue", "col")))
    return jax.shard_map(body, mesh=mesh, in_specs=in_specs, out_specs=out_specs, check_vma=False)
```

```python
import functools

import jax
import jax.numpy as jnp
from jax import lax
from jax.experimental import pallas as pl
from jax.experimental.pallas import tpu as pltpu
from jax.sharding import PartitionSpec as P

MESH = pl.DeviceIdType.MESH
F32 = jnp.float32
BF16 = jnp.bfloat16


def power_eight(corr):
    half = (1.0 + corr) * 0.5
    half = half * half
    half = half * half
    return half * half


def flip(r, d):
    out = r
    for b in range(6):
        bit = 1 << b
        out = out + ((d // bit) % 2) * (1 - 2 * ((r // bit) % 2)) * bit
    return out


def dot(a, b, dims=((1,), (0,))):
    return lax.dot_general(a, b, (dims, ((), ())), preferred_element_type=F32)


def kernel(R, C, eps, expr, win, out, dego,
           stats, zl, zcol, zrt, zw, zwr, zwt, pbuf, macc, rs, degb, degr,
           s_st, r_st, s_aa, r_aa, s_ga, r_ga, s_zc, r_zc, s_zr, r_zr,
           s_up, r_up, s_dn, r_dn, s_rs, r_rs, s_dg, r_dg):
    r = lax.axis_index("row")
    c = lax.axis_index("col")
    S, width = expr.shape
    pad = zl.shape[0]
    slab = width // R
    W = zw.shape[2]
    per = W // R
    NC, chunk = zrt.shape[1], zrt.shape[2]

    barrier = pltpu.get_barrier_semaphore()
    for d in range(1, R):
        pl.semaphore_signal(barrier, inc=1, device_id={"row": flip(r, d)}, device_id_type=MESH)
    for d in range(1, C):
        pl.semaphore_signal(barrier, inc=1, device_id={"col": lax.rem(c + d, C)}, device_id_type=MESH)

    for j in range(R):
        cols = slice(j * slab, (j + 1) * slab)
        x = expr[:, cols]
        total = jnp.sum(x, axis=0, keepdims=True)
        dev = x - total * (1.0 / S)
        stats[0, 0:1, cols] = total
        stats[0, 1:2, cols] = jnp.sum(dev * dev, axis=0, keepdims=True)
    pl.semaphore_wait(barrier, R + C - 2)

    def rowcopy(src, dst, ss, rr, d):
        return pltpu.make_async_remote_copy(
            src_ref=src, dst_ref=dst, send_sem=ss, recv_sem=rr,
            device_id={"row": flip(r, d)}, device_id_type=MESH)

    def colcopy(src, dst, ss, rr, peer):
        return pltpu.make_async_remote_copy(
            src_ref=src, dst_ref=dst, send_sem=ss, recv_sem=rr,
            device_id={"col": peer}, device_id_type=MESH)

    st = [rowcopy(stats.at[0], stats.at[d], s_st.at[d], r_st.at[d], d) for d in range(1, R)]
    for cp in st:
        cp.start()
    macc[...] = jnp.zeros_like(macc)
    zl[pad - 16:pad, :] = jnp.zeros((16, width), BF16)
    pbuf[...] = jnp.ones_like(pbuf)
    for cp in st:
        cp.wait_recv()

    for j in range(R):
        cols = slice(j * slab, (j + 1) * slab)
        total = stats[0, 0:1, cols]
        for d in range(1, R):
            total = total + stats[d, 0:1, cols]
        mean = total / (S * R)
        sq = jnp.zeros_like(mean)
        for d in range(R):
            gap = stats[d, 0:1, cols] * (1.0 / S) - mean
            sq = sq + (stats[d, 1:2, cols] + S * gap * gap)
        inv = 1.0 / jnp.sqrt(sq + eps)
        zl[0:S, cols] = ((expr[:, cols] - mean) * inv).astype(BF16)

    mine = pl.ds(pl.multiple_of(r * pad, 16), pad)
    aa = []
    for k in range(NC):
        for d in range(1, R):
            q = flip(r, d)
            at = pl.multiple_of(q * slab + k * chunk, 128)
            aa.append(rowcopy(zl.at[:, pl.ds(at, chunk)],
                              zcol.at[q, mine, k * chunk:(k + 1) * chunk],
                              s_aa.at[k, d], r_aa.at[k, d], d))
            aa[-1].start()
    zcol[r, mine, :] = zl[:, pl.ds(pl.multiple_of(r * slab, 128), slab)]

    pick = jnp.zeros((pad, W), F32)
    for j in range(R):
        gene = lax.broadcasted_iota(jnp.int32, (slab, W), 0) + (c * width + j * slab)
        onehot = jnp.where(gene == win[...], 1.0, 0.0).astype(BF16)
        pick = pick + dot(zl[:, j * slab:(j + 1) * slab], onehot)
    zw[0] = pick.astype(BF16)
    zc = []
    for d in range(1, C):
        zc.append(colcopy(zw.at[0], zw.at[d], s_zc.at[d], r_zc.at[d], lax.rem(c + d, C)))
        zc[-1].start()

    zr_own = zcol.at[r]
    lo, hi = c > 0, c < C - 1

    def up(s, k):
        i = c - s
        return colcopy(zrt.at[i, k], zrt.at[i, k], s_up.at[s, k], r_up.at[s, k], c + 1)

    def up_in(s, k):
        i = c - s
        return colcopy(zrt.at[i, k], zrt.at[i, k], s_up.at[s - 1, k], r_up.at[s - 1, k], c + 1)

    def down(s, k):
        i = c + s
        return colcopy(zrt.at[i, k], zrt.at[i, k], s_dn.at[s, k], r_dn.at[s, k], c - 1)

    def down_in(s, k):
        i = c + s
        return colcopy(zrt.at[i, k], zrt.at[i, k], s_dn.at[s - 1, k], r_dn.at[s - 1, k], c - 1)

    for k in range(NC):
        for cp in aa[k * (R - 1):(k + 1) * (R - 1)]:
            cp.wait_recv()
        zrt[c, k] = zr_own[:, k * chunk:(k + 1) * chunk].T

        @pl.when(hi)
        def _():
            up(0, k).start()

        @pl.when(lo)
        def _():
            down(0, k).start()

    relay = R == 4

    def gather(k, d):
        piece = zcol.at[r, :, pl.ds(pl.multiple_of(k * chunk, 128), chunk)]
        return rowcopy(piece, piece, s_ga.at[k, d], r_ga.at[k, d], d)

    def forward(k, via, to):
        piece = zcol.at[flip(r, via), :, pl.ds(pl.multiple_of(k * chunk, 128), chunk)]
        return rowcopy(piece, piece, s_ga.at[k, R - 1], r_ga.at[k, R - 1], to)

    direct = R - 1 if relay else R
    for d in range(1, direct):
        gather(0, d).start()

    tot = zw[0].astype(F32)
    for cp in zc:
        cp.wait_recv()
    for d in range(1, C):
        tot = tot + zw[d].astype(F32)
    zwr[0] = tot.astype(BF16)
    zr = []
    for d in range(1, R):
        zr.append(rowcopy(zwr.at[0], zwr.at[d], s_zr.at[d], r_zr.at[d], d))
        zr[-1].start()
    for k in range(1, NC):
        for d in range(1, direct):
            gather(k, d).start()
    for cp in zr:
        cp.wait_recv()
    for d in range(R):
        zwt[pl.ds(pl.multiple_of(flip(r, d) * pad, 16), pad), :] = zwr[d]

    def compute(i, k, d_lo, d_hi):
        def one(d, _):
            j = flip(r, d)
            adj = power_eight(dot(zrt[i, k], zcol[j])).astype(BF16)
            macc[j] += dot(pbuf[i, k], adj)
            return 0
        lax.fori_loop(d_lo, d_hi, one, 0)

    def panel(i, k):
        pt = power_eight(dot(zrt[i, k], zwt[...])).T
        pbuf[i, k, 0:W, :] = pt.astype(BF16)

    def arrive(s, k):
        @pl.when(c - s >= 0)
        def _():
            up_in(s, k).wait_recv()

            @pl.when(hi)
            def _():
                up(s, k).start()

        @pl.when(c + s < C)
        def _():
            down_in(s, k).wait_recv()

            @pl.when(lo)
            def _():
                down(s, k).start()

    def phase(s, t_lo, t_hi, start, d_hi):
        def step(k, _):
            arrive(s, k)

            def each(t, _):
                i = c + (1 - 2 * (t % 2)) * ((t + 1) // 2)

                @pl.when((i >= 0) & (i < C))
                def _():
                    @pl.when(start(t) == 0)
                    def _():
                        panel(i, k)
                    compute(i, k, start(t), d_hi)
                return 0
            lax.fori_loop(t_lo, t_hi, each, 0)
            return 0
        lax.fori_loop(0, NC, step, 0)

    def own(k, _):
        panel(c, k)
        compute(c, k, 0, 1)
        return 0
    lax.fori_loop(0, NC, own, 0)

    for k in range(NC):
        arrive(1, k)
        for d in range(1, R - 1):
            gather(k, d).wait_recv()
        if relay:
            via = 1 if k < NC // 2 else 2
            forward(k, via, 3 - via).start()
    phase(2, 0, 3, lambda t: jnp.where(t == 0, 1, 0), R - 1)
    for k in range(NC):
        gather(k, R - 1).wait_recv()
    phase(3, 0, 7, lambda t: jnp.where(t < 3, R - 1, 0), R)
    if C > 4:
        def later(s, _):
            phase(s, 2 * s - 1, 2 * s + 1, lambda t: 0, R)
            return 0
        lax.fori_loop(4, C, later, 0)

    out_cp = []
    for d in range(1, R):
        q = pl.multiple_of(flip(r, d) * per, 8)
        for j in range(R):
            out_cp.append(rowcopy(macc.at[j, pl.ds(q, per), :], rs.at[d, j],
                                  s_rs.at[d, j], r_rs.at[d, j], d))
            out_cp[-1].start()
    for j in range(R):
        degb[j] = macc[j, W:W + 1, :]
    zs = zcol[r].astype(F32)
    self_term = power_eight(jnp.sum(zs * zs, axis=0, keepdims=True))
    degb[r] = degb[r] - self_term.astype(BF16).astype(F32)
    dg = []
    for d in range(1, R):
        dg.append(rowcopy(degb, degr.at[d], s_dg.at[d], r_dg.at[d], d))
        dg[-1].start()
    own_rows = pl.ds(pl.multiple_of(r * per, 8), per)
    for j in range(R):
        total = macc[j, own_rows, :]
        for d in range(1, R):
            out_cp[(d - 1) * R + j].wait_recv()
            total = total + rs[d, j]
        out[:, j * slab:(j + 1) * slab] = total
    for cp in dg:
        cp.wait_recv()
    for j in range(R):
        total = degb[j]
        for d in range(1, R):
            total = total + degr[d, j]
        dego[:, j * slab:(j + 1) * slab] = total

    for cp in st + aa + zc + zr + out_cp + dg:
        cp.wait_send()
    for k in range(NC):
        for d in range(1, R):
            gather(k, d).wait_send()

    def drain(s, _):
        def each(k, _):
            @pl.when(hi & (c - s >= 0))
            def _():
                up(s, k).wait_send()

            @pl.when(lo & (c + s < C))
            def _():
                down(s, k).wait_send()
            return 0
        lax.fori_loop(0, NC, each, 0)
        return 0
    lax.fori_loop(0, C - 1, drain, 0)


def solution(mesh):
    R, C = mesh.shape["row"], mesh.shape["col"]

    def body(expr, win):
        S, width = expr.shape
        W = win.shape[0]
        pad = (S + 15) // 16 * 16
        slab = width // R
        chunk = min(256, slab)
        NC = slab // chunk
        V = pltpu.VMEM
        dma = pltpu.SemaphoreType.DMA
        vm = pl.BlockSpec(memory_space=pltpu.VMEM)
        margin, degree = pl.pallas_call(
            functools.partial(kernel, R, C, 1e-6),
            out_shape=(jax.ShapeDtypeStruct((W // R, width), F32),
                       jax.ShapeDtypeStruct((1, width), F32)),
            in_specs=[vm, vm],
            out_specs=(vm, vm),
            scratch_shapes=[
                V((R, 2, width), F32),
                V((pad, width), BF16),
                V((R, R * pad, slab), BF16),
                V((C, NC, chunk, R * pad), BF16),
                V((C, pad, W), BF16),
                V((R, pad, W), BF16),
                V((R * pad, W), BF16),
                V((C, NC, W + 16, chunk), BF16),
                V((R, W + 16, slab), F32),
                V((R, R, W // R, slab), F32),
                V((R, 1, slab), F32),
                V((R, R, 1, slab), F32),
                dma((R,)), dma((R,)), dma((NC, R)), dma((NC, R)), dma((NC, R)), dma((NC, R)),
                dma((C,)), dma((C,)), dma((R,)), dma((R,)),
                dma((C, NC)), dma((C, NC)), dma((C, NC)), dma((C, NC)),
                dma((R, R)), dma((R, R)), dma((R,)), dma((R,)),
            ],
            compiler_params=pltpu.CompilerParams(
                collective_id=0, has_side_effects=True, vmem_limit_bytes=56 << 20),
        )(expr, win.reshape(1, W))
        return margin, degree.reshape(width)

    in_specs = (P(("tissue", "row"), "col"), P())
    out_specs = (P(("tissue", "row"), "col"), P(("tissue", "col")))
    return jax.shard_map(body, mesh=mesh, in_specs=in_specs, out_specs=out_specs, check_vma=False)
```
